32 devices in a mesh: dp: 2 (over x), row: 4 (over z), col: 4 (over y, core).
Axes of the slice: x: 2, y: 2, z: 4, core: 2. Of those that a mesh axis runs over, the one named last changes fastest.
Arguments:
- history: bfloat16 [4, 4096, 2048], P(None, ('dp', 'row'), 'col'), may hold values from -6 to 6
- segment_ids: int32 [8, 512], P(('dp', 'col')), may hold values from 0 to 21, as said below
- position_ids: int32 [8, 512], P(('dp', 'col')), may hold values from 0 to 199, as said below
- mix_gain: bfloat16 [2048], P('col'), may hold values from 0.5 to 1.5
- mix_in: bfloat16 [2048, 16], P('col'), may hold values from -0.125 to 0.125
- mix_out: bfloat16 [16, 16], replicated, may hold values from -1.5 to 1.5
- mix_bias: bfloat16 [16], replicated, may hold values from -3 to 3
- lane_gain: bfloat16 [3, 2048], P(None, 'col'), may hold values from 0.5 to 1.5
- lane_bias: bfloat16 [3, 2048], P(None, 'col'), may hold values from -2 to 2
- qkv_weight: bfloat16 [3, 2048, 2048], P(None, 'col', 'row'), may hold values from -0.125 to 0.125
- qkv_bias: bfloat16 [3, 2048], P(None, 'row'), may hold values from -2 to 2
- proj_weight: bfloat16 [2048, 2048], P('row', 'col'), may hold values from -0.5 to 0.5
- proj_bias: bfloat16 [2048], P('col'), may hold values from -2 to 2
- ffn_norm_gain: bfloat16 [2048], P('col'), may hold values from 0.5 to 1.5
- feedforward_norm_bias: bfloat16 [2048], P('col'), may hold values from -2 to 2
- up_weight: bfloat16 [2048, 8192], P('col', 'row'), may hold values from -0.125 to 0.125
- up_bias: bfloat16 [8192], P('row'), may hold values from -2 to 2
- down_weight: bfloat16 [8192, 2048], P('row', 'col'), may hold values from -0.0625 to 0.0625
- down_bias: bfloat16 [2048], P('col'), may hold values from -2 to 2
- cotangent: bfloat16 [4096, 2048], P(('dp', 'row'), 'col'), may hold values from -6 to 6
Outputs:
- layer_out: bfloat16 [4096, 2048], P(('dp', 'row'), 'col')
- history_grad: float32 [4, 4096, 2048], P(None, ('dp', 'row'), 'col')
- mix_gain_grad: float32 [2048], P('col')
- mix_in_grad: float32 [2048, 16], P('col')
- mix_out_grad: float32 [16, 16], replicated
- mix_bias_grad: float32 [16], replicated
- lane_gain_grad: float32 [3, 2048], P(None, 'col')
- lane_bias_grad: float32 [3, 2048], P(None, 'col')
- qkv_weight_grad: float32 [3, 2048, 2048], P(None, 'col', 'row')
- qkv_bias_grad: float32 [3, 2048], P(None, 'row')
- proj_weight_grad: float32 [2048, 2048], P('row', 'col')
- proj_bias_grad: float32 [2048], P('col')
- feedforward_norm_gain_gradient: float32 [2048], P('col')
- ffn_norm_bias_grad: float32 [2048], P('col')
- up_weight_grad: float32 [2048, 8192], P('col', 'row')
- up_bias_grad: float32 [8192], P('row')
- down_weight_grad: float32 [8192, 2048], P('row', 'col')
- down_bias_grad: float32 [2048], P('col')
The draws below stay inside these ranges and needn't reach their ends.
Inputs may be any that keep to these rules, and one draw needn't show every extreme that they name: `segment_ids`: in each packed sequence of 512 tokens documents are numbered from 0 and the numbers never fall; a document has at most 200 tokens, and every one but the last of its sequence has 15 or more. `position_ids`: each token's place within its document, counted from 0 at the document's first token.
All inputs are finite; a program needn't handle non-finite values.
Results may differ from the reference program's by a relative error of at most 0.033.
Values may be sent and summed in bfloat16 or wider, within the bound.
A program may use at most 256 MiB of HBM per device.

```python
import math
import jax
import jax.numpy as jnp
from jax import lax

MODEL_WIDTH = 2048
HEADS = 16
HEAD_DIM = 128
FF = 8192
MIX_HID = 16
SOURCES = 4
SEQ = 512
NSEQ = 8
TOKENS = 4096
DOC_MIN = 15
DOC_MAX = 200


def doc_layout(key):
    slot_count = SEQ // DOC_MIN + 2
    lengths = jax.random.randint(jax.random.fold_in(key, 11), (NSEQ, slot_count), DOC_MIN, DOC_MAX + 1, dtype=jnp.int32)
    longest = jax.random.randint(jax.random.fold_in(key, 12), (NSEQ, 1), 0, 2, dtype=jnp.int32)
    seq_index = jnp.arange(NSEQ, dtype=jnp.int32)[:, None]
    slot_index = jnp.arange(slot_count, dtype=jnp.int32)[None, :]
    longest = jnp.where(seq_index == 0, 0, longest)
    lengths = jnp.where(seq_index == 0, DOC_MIN, lengths)
    lengths = jnp.where(slot_index == longest, DOC_MAX, lengths)
    doc_ends = jnp.cumsum(lengths, axis=1, dtype=jnp.int32)
    starts = doc_ends - lengths
    places = jnp.arange(SEQ, dtype=jnp.int32)
    segments = jnp.sum((doc_ends[:, None, :] <= places[None, :, None]).astype(jnp.int32), axis=2)
    begins = jnp.max(jnp.where(starts[:, None, :] <= places[None, :, None], starts[:, None, :], 0), axis=2)
    return (segments.astype(jnp.int32), (places[None, :] - begins).astype(jnp.int32))


def draw_segment_ids(key, part):
    return doc_layout(key)[0]


def draw_position_ids(key, part):
    return doc_layout(key)[1]


def shard_levels(own_key, shape, pieces, smallest, high):
    def one(dim, blocks):
        steps = jax.random.uniform(jax.random.fold_in(jax.random.fold_in(own_key, 6), dim), (blocks,), jnp.float32, smallest / len(pieces), high / len(pieces))
        return jnp.repeat(jnp.exp(steps), shape[dim] // blocks).reshape((-1,) + (1,) * (len(shape) - dim - 1))

    factor_of = one(*pieces[0])
    for cut in pieces[1:]:
        factor_of = factor_of * one(*cut)
    return factor_of


def normal_values(rng, dims, scale, most, split=(), kind=jnp.bfloat16):
    array = jax.random.normal(rng, dims, jnp.float32) * scale
    if len(split) > 0:
        array = shard_levels(rng, dims, split, -0.22, 0.18) * array
    return jnp.clip(array, min=-most, max=most).astype(kind)


def setup_inputs(seed: int = 0) -> dict:
    key_of = jax.random.split(jax.random.key(seed), 21)
    history = normal_values(key_of[0], (SOURCES, TOKENS, MODEL_WIDTH), 1.0, 6.0, ((1, 8), (2, 4)))
    segment_ids = draw_segment_ids(jax.random.fold_in(key_of[20], 71), 0)
    position_ids = draw_position_ids(jax.random.fold_in(key_of[20], 71), 0)
    mix_gain = jnp.clip(1.0 + 0.1 * jax.random.normal(key_of[3], (MODEL_WIDTH,), jnp.float32), 0.5, 1.5).astype(jnp.bfloat16)
    mix_in = normal_values(key_of[4], (MODEL_WIDTH, MIX_HID), MODEL_WIDTH ** -0.5, 0.125, ((0, 4),))
    mix_out = normal_values(key_of[5], (MIX_HID, 4 * SOURCES), MIX_HID ** -0.5, 1.5)
    mix_bias = normal_values(key_of[6], (4 * SOURCES,), 0.5, 3.0)
    lane_gain = jnp.clip(1.0 + 0.1 * jax.random.normal(key_of[7], (3, MODEL_WIDTH), jnp.float32), 0.5, 1.5).astype(jnp.bfloat16)
    lane_bias = normal_values(key_of[8], (3, MODEL_WIDTH), 0.3, 2.0, ((1, 4),))
    qkv_weight = normal_values(key_of[9], (3, MODEL_WIDTH, MODEL_WIDTH), MODEL_WIDTH ** -0.5, 0.125, ((1, 4), (2, 4)))
    qkv_bias = normal_values(key_of[10], (3, MODEL_WIDTH), 0.3, 2.0, ((1, 4),))
    proj_weight = normal_values(key_of[11], (MODEL_WIDTH, MODEL_WIDTH), (MODEL_WIDTH // 16) ** -0.5, 0.5, ((0, 4), (1, 4)))
    proj_bias = normal_values(key_of[12], (MODEL_WIDTH,), 0.3, 2.0, ((0, 4),))
    ffn_norm_gain = jnp.clip(1.0 + 0.1 * jax.random.normal(key_of[13], (MODEL_WIDTH,), jnp.float32), 0.5, 1.5).astype(jnp.bfloat16)
    feedforward_norm_bias = normal_values(key_of[14], (MODEL_WIDTH,), 0.3, 2.0, ((0, 4),))
    up_weight = normal_values(key_of[15], (MODEL_WIDTH, FF), MODEL_WIDTH ** -0.5, 0.125, ((0, 4), (1, 4)))
    up_bias = normal_values(key_of[16], (FF,), 0.3, 2.0, ((0, 4),))
    down_weight = normal_values(key_of[17], (FF, MODEL_WIDTH), FF ** -0.5, 0.0625, ((0, 4), (1, 4)))
    down_bias = normal_values(key_of[18], (MODEL_WIDTH,), 0.3, 2.0, ((0, 4),))
    cotangent = normal_values(key_of[19], (TOKENS, MODEL_WIDTH), 1.0, 6.0, ((0, 8), (1, 4)))
    return dict(history=history, segment_ids=segment_ids, position_ids=position_ids, mix_gain=mix_gain, mix_in=mix_in, mix_out=mix_out, mix_bias=mix_bias, lane_gain=lane_gain, lane_bias=lane_bias, qkv_weight=qkv_weight, qkv_bias=qkv_bias, proj_weight=proj_weight, proj_bias=proj_bias, ffn_norm_gain=ffn_norm_gain, feedforward_norm_bias=feedforward_norm_bias, up_weight=up_weight, up_bias=up_bias, down_weight=down_weight, down_bias=down_bias, cotangent=cotangent)


@jax.custom_vjp
def low(v):
    return lax.optimization_barrier(v.astype(jnp.bfloat16)).astype(jnp.float32)

@jax.custom_vjp
def low_back(v):
    return v

def low_keep(v):
    return (low(v), None)

def low_pass(kept, grad):
    return (grad,)

def back_keep(v):
    return (v, None)

def back_low(kept, grad):
    return (low(grad),)
low.defvjp(low_keep, low_pass)
low_back.defvjp(back_keep, back_low)
norm_eps = 1e-05
mix_eps = 1e-06
masked_score = -1e+30
highest = lax.Precision.HIGHEST

def exact_gelu(inputs):
    return jax.nn.gelu(inputs, approximate=False)

def rotary_tables(places):
    half_rot = HEAD_DIM // 8
    inverse_freq = jnp.exp(jnp.arange(half_rot, dtype=jnp.float32) * (-2.0 * math.log(10000.0) / (2 * half_rot)))
    angles = places.astype(jnp.float32)[:, None] * inverse_freq[None, :]
    return (jnp.cos(angles)[:, None, :], jnp.sin(angles)[:, None, :])

def rotate(vectors, cosine, sine, direction):
    half_rot = HEAD_DIM // 8
    lead_part = vectors[..., :half_rot]
    pair_part = vectors[..., half_rot:2 * half_rot]
    rest_part = vectors[..., 2 * half_rot:]
    return jnp.concatenate([lead_part * cosine - direction * (pair_part * sine), pair_part * cosine + direction * (lead_part * sine), rest_part], axis=-1)

def layer_norm(values, norm_gain, shift):
    center = lax.optimization_barrier(jnp.mean(values, axis=-1, keepdims=True))
    deviation = values - center
    variance = lax.optimization_barrier(jnp.mean(deviation * deviation, axis=-1, keepdims=True))
    return deviation * lax.rsqrt(variance + norm_eps) * norm_gain + shift

def attend_sequence(packed):
    query, key_rows, value_rows, seg_row = packed
    scores = low_back(jnp.einsum('qhd,khd->hqk', query, key_rows, precision=highest) * HEAD_DIM ** (-0.5))
    places = jnp.arange(seg_row.shape[0], dtype=jnp.int32)
    allowed = (seg_row[:, None] == seg_row[None, :]) & (places[None, :] <= places[:, None])
    attn_probs = jax.nn.softmax(jnp.where(allowed[None], scores, masked_score), axis=-1)
    return jnp.einsum('hqk,khd->qhd', low(attn_probs), value_rows, precision=highest)

def layer_forward(weights, hist, seg_group, pos_group):
    mix_gain, mix_in, mix_out, mix_bias, lane_gain, lane_bias, qkv_weight, qkv_bias, proj_weight, proj_bias, ffn_norm_gain, feedforward_norm_bias, up_weight, up_bias, down_weight, down_bias = weights
    latest = hist[SOURCES - 1]
    tok_count = latest.shape[0]
    mean_square = lax.optimization_barrier(jnp.mean(latest * latest, axis=-1, keepdims=True))
    normed_mix = latest * lax.rsqrt(mean_square + mix_eps) * mix_gain
    mix_pre = jnp.dot(normed_mix, mix_in, precision=highest)
    coeffs = (jnp.dot(exact_gelu(mix_pre), mix_out, precision=highest) + mix_bias).reshape(tok_count, 4, SOURCES)
    input_streams = jnp.einsum('tsj,jtd->std', coeffs, hist, precision=highest)
    projected = []
    for stream_index in range(3):
        normed_in = low(layer_norm(input_streams[stream_index], lane_gain[stream_index], lane_bias[stream_index]))
        projected.append(low_back(jnp.dot(normed_in, qkv_weight[stream_index], precision=highest) + qkv_bias[stream_index]))
    cosine, sine = rotary_tables(pos_group.reshape(tok_count))
    head_shape = (tok_count, HEADS, HEAD_DIM)
    seq_shape = (seg_group.shape[0], seg_group.shape[1], HEADS, HEAD_DIM)
    query = low(rotate(projected[0].reshape(head_shape), cosine, sine, 1.0)).reshape(seq_shape)
    key_rows = low(rotate(projected[1].reshape(head_shape), cosine, sine, 1.0)).reshape(seq_shape)
    value_rows = low(projected[2]).reshape(seq_shape)
    attended = lax.map(jax.checkpoint(attend_sequence), (query, key_rows, value_rows, seg_group))
    attn_round = low(low_back(attended.reshape(tok_count, MODEL_WIDTH)))
    residual_stream = input_streams[3] + low_back(jnp.dot(attn_round, proj_weight, precision=highest) + proj_bias)
    feedforward_input = low(layer_norm(residual_stream, ffn_norm_gain, feedforward_norm_bias))
    up_pre = low_back(jnp.dot(feedforward_input, up_weight, precision=highest) + up_bias)
    up_act = low(exact_gelu(up_pre))
    return residual_stream + jnp.dot(up_act, down_weight, precision=highest) + down_bias

def reference(history, segment_ids, position_ids, mix_gain, mix_in, mix_out, mix_bias, lane_gain, lane_bias, qkv_weight, qkv_bias, proj_weight, proj_bias, ffn_norm_gain, feedforward_norm_bias, up_weight, up_bias, down_weight, down_bias, cotangent):
    weights = tuple((weight_arg.astype(jnp.float32) for weight_arg in (mix_gain, mix_in, mix_out, mix_bias, lane_gain, lane_bias, qkv_weight, qkv_bias, proj_weight, proj_bias, ffn_norm_gain, feedforward_norm_bias, up_weight, up_bias, down_weight, down_bias)))
    group_seqs = max(1, min(NSEQ, 4096 // SEQ))
    while NSEQ % group_seqs != 0:
        group_seqs = group_seqs - 1
    group_count = NSEQ // group_seqs
    group_len = group_seqs * SEQ
    hist_groups = history.reshape(SOURCES, group_count, group_len, MODEL_WIDTH).transpose(1, 0, 2, 3)
    seg_groups = segment_ids.reshape(group_count, group_seqs, SEQ)
    pos_groups = position_ids.reshape(group_count, group_seqs, SEQ)
    cot_groups = cotangent.reshape(group_count, group_len, MODEL_WIDTH)

    def group_step(totals, packed):
        hist_group, seg_group, pos_group, cot_group = packed

        def forward(weight_set, hist_float):
            return layer_forward(weight_set, hist_float, seg_group, pos_group)
        out_value, pull_back = jax.vjp(forward, weights, hist_group.astype(jnp.float32))
        weight_grads, hist_grad = pull_back(cot_group.astype(jnp.float32))
        totals = jax.tree.map(lambda left, right: left + right, totals, weight_grads)
        return (totals, (out_value.astype(jnp.bfloat16), hist_grad))
    zero_grads = jax.tree.map(jnp.zeros_like, weights)
    grad_totals, (out_groups, hist_grads) = lax.scan(group_step, zero_grads, (hist_groups, seg_groups, pos_groups, cot_groups))
    mix_gain_grad, mix_in_grad, mix_out_grad, mix_bias_grad, lane_gain_grad, lane_bias_grad, qkv_weight_grad, qkv_bias_grad, proj_weight_grad, proj_bias_grad, feedforward_norm_gain_gradient, ffn_norm_bias_grad, up_weight_grad, up_bias_grad, down_weight_grad, down_bias_grad = grad_totals
    layer_out = out_groups.reshape(TOKENS, MODEL_WIDTH)
    history_grad = hist_grads.transpose(1, 0, 2, 3).reshape(SOURCES, TOKENS, MODEL_WIDTH)
    return (layer_out, history_grad, mix_gain_grad, mix_in_grad, mix_out_grad, mix_bias_grad, lane_gain_grad, lane_bias_grad, qkv_weight_grad, qkv_bias_grad, proj_weight_grad, proj_bias_grad, feedforward_norm_gain_gradient, ffn_norm_bias_grad, up_weight_grad, up_bias_grad, down_weight_grad, down_bias_grad)
```

```python
import functools
import math

import jax
import jax.numpy as jnp
from jax import lax
from jax.experimental import pallas as pl
from jax.experimental.pallas import tpu as pltpu
from jax.sharding import PartitionSpec as P

MODEL_WIDTH = 2048
HEAD_DIM = 128
MIX_HID = 16
SOURCES = 4


norm_eps = 1e-05
mix_eps = 1e-06
masked_score = -1e30
highest = lax.Precision.HIGHEST


def exact_gelu(inputs):
    return jax.nn.gelu(inputs, approximate=False)


def rotary_tables(places):
    half_rot = HEAD_DIM // 8
    inverse_freq = jnp.exp(
        jnp.arange(half_rot, dtype=jnp.float32) * (-2.0 * math.log(10000.0) / (2 * half_rot))
    )
    angles = places.astype(jnp.float32)[:, None] * inverse_freq[None, :]
    return (jnp.cos(angles)[:, None, :], jnp.sin(angles)[:, None, :])


def rotate(vectors, cosine, sine, direction):
    half_rot = HEAD_DIM // 8
    lead_part = vectors[..., :half_rot]
    pair_part = vectors[..., half_rot : 2 * half_rot]
    rest_part = vectors[..., 2 * half_rot :]
    return jnp.concatenate(
        [
            lead_part * cosine - direction * (pair_part * sine),
            pair_part * cosine + direction * (lead_part * sine),
            rest_part,
        ],
        axis=-1,
    )


def feature_sums(stats):
    return lax.psum(stats, "col")


def gather_rows(stacked):
    return lax.all_gather(stacked, "row", axis=1, tiled=True)


def gather_cols(stacked):
    return lax.all_gather(stacked, "col", axis=1, tiled=True)


def sum_over_cols(gathered_list, term_fn):

    def term_rows(first_row, row_count):
        return term_fn([gathered for gathered in gathered_list])

    return lax.psum_scatter(
        term_rows(
            jnp.int32(0), lax.axis_size("col") * (gathered_list[0].shape[1] // lax.axis_size("col"))
        ).astype(jnp.bfloat16),
        "col",
        scatter_dimension=0,
        tiled=True,
    ).astype(jnp.float32)


def sum_over_rows(gathered_list, term_fn):

    def term_rows(first_row, row_count):
        return term_fn([gathered for gathered in gathered_list])

    return lax.psum_scatter(
        term_rows(
            jnp.int32(0), lax.axis_size("row") * (gathered_list[0].shape[1] // lax.axis_size("row"))
        ).astype(jnp.bfloat16),
        "row",
        scatter_dimension=0,
        tiled=True,
    ).astype(jnp.float32)


def apply_layer_norm(values, total, square):
    mean_val = total / MODEL_WIDTH
    inverse_deviation = lax.rsqrt(square / MODEL_WIDTH - mean_val * mean_val + norm_eps)
    return ((values - mean_val[:, None]) * inverse_deviation[:, None], inverse_deviation)


def layer_norm_backward(
    output_gradient,
    centered_unit,
    inverse_deviation,
    norm_gain,
    leading_reduction_sum,
    trailing_reduction_sum,
):
    scaled_normed = output_gradient * norm_gain
    return inverse_deviation[:, None] * (
        scaled_normed
        - leading_reduction_sum[:, None] / MODEL_WIDTH
        - centered_unit * (trailing_reduction_sum[:, None] / MODEL_WIDTH)
    )


def score_block(query_block, key_rows, seg_block, seg_all, first_row):
    scores = jnp.einsum(
        "qhd,khd->hqk", query_block, key_rows, preferred_element_type=jnp.float32
    ) * HEAD_DIM ** (-0.5)
    query_place = first_row + jnp.arange(query_block.shape[0], dtype=jnp.int32)
    key_place = jnp.arange(key_rows.shape[0], dtype=jnp.int32)
    allowed = (seg_block[:, None] == seg_all[None, :]) & (
        key_place[None, :] <= query_place[:, None]
    )
    return jnp.where(allowed[None], scores, masked_score)


def attend_forward(query, key_rows, value_rows, seg_all):
    seq_span = query.shape[0]
    block_len = min(512, seq_span)

    def one_block(block_index):
        first_row = block_index * block_len
        query_block = lax.dynamic_slice_in_dim(query, first_row, block_len, 0)
        seg_block = lax.dynamic_slice_in_dim(seg_all, first_row, block_len, 0)
        scores = score_block(query_block, key_rows, seg_block, seg_all, first_row)
        row_max = jnp.max(scores, axis=2, keepdims=True)
        exp_scores = jnp.exp(scores - row_max)
        row_total = jnp.sum(exp_scores, axis=2, keepdims=True)
        probs_low = (exp_scores / row_total).astype(jnp.bfloat16)
        result = jnp.einsum(
            "hqk,khd->qhd", probs_low, value_rows, preferred_element_type=jnp.float32
        )
        return (result, row_max, row_total)

    results, row_maxes, row_totals = lax.map(
        one_block, jnp.arange(seq_span // block_len, dtype=jnp.int32)
    )
    return (results.reshape(query.shape), row_maxes, row_totals)


def attend_backward(query, key_rows, value_rows, seg_all, output_gradient, row_maxes, row_totals):
    seq_span = query.shape[0]
    block_len = min(512, seq_span)
    scale = HEAD_DIM ** (-0.5)

    def one_block(carry, block_index):
        key_grad, value_grad = carry
        first_row = block_index * block_len
        query_block = lax.dynamic_slice_in_dim(query, first_row, block_len, 0)
        seg_block = lax.dynamic_slice_in_dim(seg_all, first_row, block_len, 0)
        grad_block = lax.dynamic_slice_in_dim(output_gradient, first_row, block_len, 0)
        scores = score_block(query_block, key_rows, seg_block, seg_all, first_row)
        attn_probs = jnp.exp(scores - row_maxes[block_index]) / row_totals[block_index]
        probs_low = attn_probs.astype(jnp.bfloat16)
        probs_grad = jnp.einsum(
            "qhd,khd->hqk", grad_block, value_rows, preferred_element_type=jnp.float32
        )
        row_delta = jnp.sum(probs_grad * attn_probs, axis=2, keepdims=True)
        score_grad = (attn_probs * (probs_grad - row_delta)).astype(jnp.bfloat16)
        query_grad = (
            jnp.einsum("hqk,khd->qhd", score_grad, key_rows, preferred_element_type=jnp.float32)
            * scale
        )
        key_grad = (
            key_grad
            + jnp.einsum(
                "hqk,qhd->khd", score_grad, query_block, preferred_element_type=jnp.float32
            )
            * scale
        )
        value_grad = value_grad + jnp.einsum(
            "hqk,qhd->khd", probs_low, grad_block, preferred_element_type=jnp.float32
        )
        return ((key_grad, value_grad), query_grad)

    zero_grad = jnp.zeros(key_rows.shape, jnp.float32)
    (key_grad, value_grad), query_grads = lax.scan(
        one_block, (zero_grad, zero_grad), jnp.arange(seq_span // block_len, dtype=jnp.int32)
    )
    return (query_grads.reshape(query.shape), key_grad, value_grad)


def general_body(
    history,
    segment_ids,
    position_ids,
    mix_gain,
    mix_in,
    mix_out,
    mix_bias,
    lane_gain,
    lane_bias,
    qkv_weight,
    qkv_bias,
    proj_weight,
    proj_bias,
    ffn_norm_gain,
    feedforward_norm_bias,
    up_weight,
    up_bias,
    down_weight,
    down_bias,
    cotangent,
):
    tok_rows = history.shape[1]
    seq_count = segment_ids.shape[0]
    seq_len = segment_ids.shape[1]
    group_rows = seq_count * seq_len
    head_cols = qkv_weight.shape[2]
    heads_local = head_cols // HEAD_DIM
    head_shape = (group_rows, heads_local, HEAD_DIM)
    seq_shape = (seq_count, seq_len, heads_local, HEAD_DIM)
    latest = history[SOURCES - 1].astype(jnp.float32)
    gain_mix = mix_gain.astype(jnp.float32)
    weight_mix = mix_in.astype(jnp.float32)
    mixer_out = mix_out.astype(jnp.float32)
    first_stats = jnp.concatenate(
        [
            jnp.dot(latest * gain_mix, weight_mix, precision=highest).T,
            jnp.sum(latest * latest, axis=1)[None, :],
        ],
        axis=0,
    )
    first_stats = feature_sums(first_stats)
    mix_scale = lax.rsqrt(first_stats[MIX_HID] / MODEL_WIDTH + mix_eps)
    mix_pre = first_stats[:MIX_HID].T * mix_scale[:, None]
    mix_hidden, mix_gelu_back = jax.vjp(exact_gelu, mix_pre)
    coeffs = (
        jnp.dot(mix_hidden, mixer_out, precision=highest) + mix_bias.astype(jnp.float32)
    ).reshape(tok_rows, 4, SOURCES)
    input_streams = []
    for stream_index in range(4):
        mixed = coeffs[:, stream_index, 0:1] * history[0].astype(jnp.float32)
        for source in range(1, SOURCES):
            mixed = mixed + coeffs[:, stream_index, source : source + 1] * history[source].astype(
                jnp.float32
            )
        input_streams.append(mixed)
    gain_per_stream = lane_gain.astype(jnp.float32)
    bias_per_stream = lane_bias.astype(jnp.float32)
    layer_norm_statistics = feature_sums(
        jnp.stack(
            [jnp.sum(input_streams[stream_index], axis=1) for stream_index in range(3)]
            + [
                jnp.sum(input_streams[stream_index] * input_streams[stream_index], axis=1)
                for stream_index in range(3)
            ],
            axis=0,
        )
    )
    centered_unit_list = []
    inv_stds = []
    stream_inputs = []
    for stream_index in range(3):
        centered_unit, inverse_deviation = apply_layer_norm(
            input_streams[stream_index],
            layer_norm_statistics[stream_index],
            layer_norm_statistics[3 + stream_index],
        )
        centered_unit_list.append(centered_unit)
        inv_stds.append(inverse_deviation)
        stream_inputs.append(
            (centered_unit * gain_per_stream[stream_index] + bias_per_stream[stream_index]).astype(
                jnp.bfloat16
            )
        )
    inputs_gathered = [gather_rows(stream_inputs[stream_index][None]) for stream_index in range(3)]

    def qkv_term(pieces):
        return jnp.stack(
            [
                jnp.dot(
                    pieces[stream_index][0],
                    qkv_weight[stream_index],
                    preferred_element_type=jnp.float32,
                )
                for stream_index in range(3)
            ],
            axis=1,
        )

    qkv_pre = sum_over_cols(inputs_gathered, qkv_term) + qkv_bias.astype(jnp.float32)[None]
    cosine, sine = rotary_tables(position_ids.reshape(group_rows))
    query = (
        rotate(qkv_pre[:, 0].reshape(head_shape), cosine, sine, 1.0)
        .astype(jnp.bfloat16)
        .reshape(seq_shape)
    )
    key_rows = (
        rotate(qkv_pre[:, 1].reshape(head_shape), cosine, sine, 1.0)
        .astype(jnp.bfloat16)
        .reshape(seq_shape)
    )
    value_rows = qkv_pre[:, 2].astype(jnp.bfloat16).reshape(seq_shape)
    attended, row_maxes, row_totals = lax.map(
        lambda packed: attend_forward(packed[0], packed[1], packed[2], packed[3]),
        (query, key_rows, value_rows, segment_ids),
    )
    attn_round = attended.reshape(group_rows, head_cols).astype(jnp.bfloat16)
    attn_gathered = gather_cols(attn_round[None])
    attn_proj = sum_over_rows(
        [attn_gathered],
        lambda pieces: jnp.dot(pieces[0][0], proj_weight, preferred_element_type=jnp.float32),
    )
    residual_stream = input_streams[3] + attn_proj + proj_bias.astype(jnp.float32)
    feedforward_gain = ffn_norm_gain.astype(jnp.float32)
    feedforward_norm_statistics = feature_sums(
        jnp.stack(
            [jnp.sum(residual_stream, axis=1), jnp.sum(residual_stream * residual_stream, axis=1)],
            axis=0,
        )
    )
    feedforward_centered_unit, feedforward_inverse_std = apply_layer_norm(
        residual_stream, feedforward_norm_statistics[0], feedforward_norm_statistics[1]
    )
    feedforward_input = (
        feedforward_centered_unit * feedforward_gain + feedforward_norm_bias.astype(jnp.float32)
    ).astype(jnp.bfloat16)
    ffn_gathered = gather_rows(feedforward_input[None])
    up_pre = sum_over_cols(
        [ffn_gathered],
        lambda pieces: jnp.dot(pieces[0][0], up_weight, preferred_element_type=jnp.float32),
    ) + up_bias.astype(jnp.float32)
    up_value, up_gelu_back = jax.vjp(exact_gelu, up_pre)
    up_act = up_value.astype(jnp.bfloat16)
    act_gathered = gather_cols(up_act[None])
    ffn_out = sum_over_rows(
        [act_gathered],
        lambda pieces: jnp.dot(pieces[0][0], down_weight, preferred_element_type=jnp.float32),
    )
    layer_out = (residual_stream + ffn_out + down_bias.astype(jnp.float32)).astype(jnp.bfloat16)
    grad_gathered = gather_rows(cotangent[None])
    act_grad = sum_over_cols(
        [grad_gathered],
        lambda pieces: jnp.einsum(
            "td,fd->tf", pieces[0][0], down_weight, preferred_element_type=jnp.float32
        ),
    )
    down_weight_grad = jnp.einsum(
        "tf,td->fd", act_gathered[0], grad_gathered[0], preferred_element_type=jnp.float32
    )
    down_bias_grad = jnp.sum(grad_gathered[0], axis=0, dtype=jnp.float32)
    up_grad = up_gelu_back(act_grad)[0].astype(jnp.bfloat16)
    up_gathered = gather_cols(up_grad[None])
    feedforward_input_grad = sum_over_rows(
        [up_gathered],
        lambda pieces: jnp.einsum(
            "tf,df->td", pieces[0][0], up_weight, preferred_element_type=jnp.float32
        ),
    )
    up_weight_grad = jnp.einsum(
        "td,tf->df", ffn_gathered[0], up_gathered[0], preferred_element_type=jnp.float32
    )
    up_bias_grad = jnp.sum(up_gathered[0], axis=0, dtype=jnp.float32)
    feedforward_scaled = feedforward_input_grad * feedforward_gain
    feedforward_backward = feature_sums(
        jnp.stack(
            [
                jnp.sum(feedforward_scaled, axis=1),
                jnp.sum(feedforward_scaled * feedforward_centered_unit, axis=1),
            ],
            axis=0,
        )
    )
    resid_grad = cotangent.astype(jnp.float32) + layer_norm_backward(
        feedforward_input_grad,
        feedforward_centered_unit,
        feedforward_inverse_std,
        feedforward_gain,
        feedforward_backward[0],
        feedforward_backward[1],
    )
    feedforward_norm_gain_gradient = jnp.sum(
        feedforward_input_grad * feedforward_centered_unit, axis=0
    )
    ffn_norm_bias_grad = jnp.sum(feedforward_input_grad, axis=0)
    proj_grad = resid_grad.astype(jnp.bfloat16)
    proj_gathered = gather_rows(proj_grad[None])
    attn_grad = sum_over_cols(
        [proj_gathered],
        lambda pieces: jnp.einsum(
            "td,hd->th", pieces[0][0], proj_weight, preferred_element_type=jnp.float32
        ),
    ).astype(jnp.bfloat16)
    proj_weight_grad = jnp.einsum(
        "th,td->hd", attn_gathered[0], proj_gathered[0], preferred_element_type=jnp.float32
    )
    proj_bias_grad = jnp.sum(proj_gathered[0], axis=0, dtype=jnp.float32)
    query_grads, key_grads, value_grads = lax.map(
        lambda packed: attend_backward(
            packed[0], packed[1], packed[2], packed[3], packed[4], packed[5], packed[6]
        ),
        (
            query,
            key_rows,
            value_rows,
            segment_ids,
            attn_grad.reshape(seq_shape),
            row_maxes,
            row_totals,
        ),
    )
    query_back = rotate(query_grads.reshape(head_shape), cosine, sine, -1.0).reshape(
        group_rows, head_cols
    )
    key_back = rotate(key_grads.reshape(head_shape), cosine, sine, -1.0).reshape(
        group_rows, head_cols
    )
    qkv_grad = jnp.stack(
        [query_back, key_back, value_grads.reshape(group_rows, head_cols)], axis=0
    ).astype(jnp.bfloat16)
    qkv_gathered = gather_cols(qkv_grad)
    input_gradient_list = sum_over_rows(
        [qkv_gathered],
        lambda pieces: jnp.einsum(
            "nte,nde->tnd", pieces[0], qkv_weight, preferred_element_type=jnp.float32
        ),
    )
    qkv_weight_grad = jnp.stack(
        [
            jnp.einsum(
                "td,te->de",
                inputs_gathered[stream_index][0],
                qkv_gathered[stream_index],
                preferred_element_type=jnp.float32,
            )
            for stream_index in range(3)
        ],
        axis=0,
    )
    qkv_bias_grad = jnp.sum(qkv_gathered, axis=1, dtype=jnp.float32)
    stream_scaled = [
        input_gradient_list[:, stream_index] * gain_per_stream[stream_index]
        for stream_index in range(3)
    ]
    lane_back = feature_sums(
        jnp.stack(
            [jnp.sum(stream_scaled[stream_index], axis=1) for stream_index in range(3)]
            + [
                jnp.sum(stream_scaled[stream_index] * centered_unit_list[stream_index], axis=1)
                for stream_index in range(3)
            ],
            axis=0,
        )
    )
    lane_grads = [
        layer_norm_backward(
            input_gradient_list[:, stream_index],
            centered_unit_list[stream_index],
            inv_stds[stream_index],
            gain_per_stream[stream_index],
            lane_back[stream_index],
            lane_back[3 + stream_index],
        )
        for stream_index in range(3)
    ]
    lane_grads.append(resid_grad)
    lane_gain_grad = jnp.stack(
        [
            jnp.sum(input_gradient_list[:, stream_index] * centered_unit_list[stream_index], axis=0)
            for stream_index in range(3)
        ],
        axis=0,
    )
    lane_bias_grad = jnp.stack(
        [jnp.sum(input_gradient_list[:, stream_index], axis=0) for stream_index in range(3)], axis=0
    )
    coeff_parts = jnp.stack(
        [
            jnp.sum(lane_grads[stream_index] * history[source].astype(jnp.float32), axis=1)
            for stream_index in range(4)
            for source in range(SOURCES)
        ],
        axis=0,
    )
    coeff_grad = feature_sums(coeff_parts).T
    mix_out_grad = jnp.dot(mix_hidden.T, coeff_grad, precision=highest)
    mix_bias_grad = jnp.sum(coeff_grad, axis=0)
    hidden_grad = jnp.dot(coeff_grad, mixer_out.T, precision=highest)
    pre_grad = mix_gelu_back(hidden_grad)[0]
    normed_mix = latest * mix_scale[:, None] * gain_mix
    mix_in_grad = jnp.dot(normed_mix.T, pre_grad, precision=highest)
    normed_grad = jnp.dot(pre_grad, weight_mix.T, precision=highest)
    mix_gain_grad = jnp.sum(normed_grad * latest * mix_scale[:, None], axis=0)
    weighted = normed_grad * gain_mix
    rms_back = feature_sums(jnp.sum(weighted * latest, axis=1)[None, :])
    latest_grad = (
        mix_scale[:, None] * weighted
        - latest
        * (mix_scale * mix_scale * mix_scale)[:, None]
        * (rms_back[0] / MODEL_WIDTH)[:, None]
    )
    source_grads = []
    for source in range(SOURCES):
        summed = coeffs[:, 0, source : source + 1] * lane_grads[0]
        for stream_index in range(1, 4):
            summed = (
                summed + coeffs[:, stream_index, source : source + 1] * lane_grads[stream_index]
            )
        if source == SOURCES - 1:
            summed = summed + latest_grad
        source_grads.append(summed)
    history_grad = jnp.stack(source_grads, axis=0)
    (
        down_weight_grad,
        down_bias_grad,
        up_weight_grad,
        up_bias_grad,
        proj_weight_grad,
        proj_bias_grad,
        qkv_weight_grad,
        qkv_bias_grad,
    ) = (
        lax.psum(down_weight_grad.astype(jnp.bfloat16), "dp").astype(jnp.float32),
        lax.psum(down_bias_grad.astype(jnp.bfloat16), "dp").astype(jnp.float32),
        lax.psum(up_weight_grad.astype(jnp.bfloat16), "dp").astype(jnp.float32),
        lax.psum(up_bias_grad.astype(jnp.bfloat16), "dp").astype(jnp.float32),
        lax.psum(proj_weight_grad.astype(jnp.bfloat16), "dp").astype(jnp.float32),
        lax.psum(proj_bias_grad.astype(jnp.bfloat16), "dp").astype(jnp.float32),
        lax.psum(qkv_weight_grad.astype(jnp.bfloat16), "dp").astype(jnp.float32),
        lax.psum(qkv_bias_grad.astype(jnp.bfloat16), "dp").astype(jnp.float32),
    )
    (
        mix_gain_grad,
        mix_in_grad,
        mix_out_grad,
        mix_bias_grad,
        lane_gain_grad,
        lane_bias_grad,
        feedforward_norm_gain_gradient,
        ffn_norm_bias_grad,
    ) = (
        lax.psum(mix_gain_grad.astype(jnp.bfloat16), ("dp", "row")).astype(jnp.float32),
        lax.psum(mix_in_grad.astype(jnp.bfloat16), ("dp", "row")).astype(jnp.float32),
        lax.psum(mix_out_grad.astype(jnp.bfloat16), ("dp", "row")).astype(jnp.float32),
        lax.psum(mix_bias_grad.astype(jnp.bfloat16), ("dp", "row")).astype(jnp.float32),
        lax.psum(lane_gain_grad.astype(jnp.bfloat16), ("dp", "row")).astype(jnp.float32),
        lax.psum(lane_bias_grad.astype(jnp.bfloat16), ("dp", "row")).astype(jnp.float32),
        lax.psum(feedforward_norm_gain_gradient.astype(jnp.bfloat16), ("dp", "row")).astype(
            jnp.float32
        ),
        lax.psum(ffn_norm_bias_grad.astype(jnp.bfloat16), ("dp", "row")).astype(jnp.float32),
    )
    return (
        layer_out,
        history_grad,
        mix_gain_grad,
        mix_in_grad,
        mix_out_grad,
        mix_bias_grad,
        lane_gain_grad,
        lane_bias_grad,
        qkv_weight_grad,
        qkv_bias_grad,
        proj_weight_grad,
        proj_bias_grad,
        feedforward_norm_gain_gradient,
        ffn_norm_bias_grad,
        up_weight_grad,
        up_bias_grad,
        down_weight_grad,
        down_bias_grad,
    )


MESH_ID = pl.DeviceIdType.MESH
CORE_SWAP = [(0, 1), (1, 0), (2, 3), (3, 2)]
CHIP_SWAP = [(0, 2), (2, 0), (1, 3), (3, 1)]
BOTH_SWAP = [(0, 3), (3, 0), (1, 2), (2, 1)]
PAIR_SWAP = [(0, 1), (1, 0)]


def small_sum_kernel(axis, size, value_ref, out_ref, slots, send_sem, recv_sem):
    me = lax.axis_index(axis)
    barrier = pltpu.get_barrier_semaphore()
    for step in range(1, size):
        pl.semaphore_signal(
            barrier, inc=1, device_id={axis: lax.rem(me + step, size)}, device_id_type=MESH_ID
        )
    pl.semaphore_wait(barrier, size - 1)
    copies = []
    for step in range(1, size):
        copies.append(
            pltpu.make_async_remote_copy(
                src_ref=value_ref,
                dst_ref=slots.at[step - 1],
                send_sem=send_sem.at[step - 1],
                recv_sem=recv_sem.at[step - 1],
                device_id={axis: jnp.bitwise_xor(me, step)},
                device_id_type=MESH_ID,
            )
        )
    for copy in copies:
        copy.start()
    for copy in copies:
        copy.wait()
    out_ref[...] = (value_ref[...] + slots[0]) + (slots[1] + slots[2])


def small_sum(values, collective_id):
    axis, size = "col", 4
    return pl.pallas_call(
        functools.partial(small_sum_kernel, axis, size),
        out_shape=jax.ShapeDtypeStruct(values.shape, values.dtype),
        in_specs=[pl.BlockSpec(memory_space=pltpu.VMEM)],
        out_specs=pl.BlockSpec(memory_space=pltpu.VMEM),
        scratch_shapes=[
            pltpu.VMEM((size - 1,) + values.shape, values.dtype),
            pltpu.SemaphoreType.DMA((size - 1,)),
            pltpu.SemaphoreType.DMA((size - 1,)),
        ],
        compiler_params=pltpu.CompilerParams(collective_id=collective_id, has_side_effects=True),
        name=f"small_sum_{collective_id}",
    )(values)


def swap_col(value, step):
    return lax.ppermute(value, "col", {1: CORE_SWAP, 2: CHIP_SWAP, 3: BOTH_SWAP}[step])


def swap_dp(value):
    return lax.ppermute(value, "dp", PAIR_SWAP)


def low_add(left, right):
    return (left.astype(jnp.float32) + right.astype(jnp.float32)).astype(jnp.bfloat16)


def gather_cols_relative(block):
    far = swap_col(block, 2)
    return [block, swap_col(block, 1), far, swap_col(far, 1)]


def place_blocks(blocks, col):
    out = jnp.zeros((4,) + blocks[0].shape, blocks[0].dtype)
    for step in range(4):
        out = lax.dynamic_update_index_in_dim(out, blocks[step], jnp.bitwise_xor(col, step), 0)
    return out


def pick(stacked, index):
    return lax.dynamic_index_in_dim(stacked, index, 0, keepdims=False)


def scatter_cols(blocks):
    near = low_add(blocks[0], swap_col(blocks[1], 1))
    far = low_add(blocks[2], swap_col(blocks[3], 1))
    return near.astype(jnp.float32) + swap_col(far, 2).astype(jnp.float32)


def split_tokens(block, col):
    quarters = block.reshape((4, block.shape[0] // 4, block.shape[1]))
    pieces = [pick(quarters, col)]
    for step in range(1, 4):
        pieces.append(swap_col(pick(quarters, jnp.bitwise_xor(col, step)), step))
    return jnp.concatenate(pieces, axis=1)


def join_tokens(quarter, col):
    rows, width = quarter.shape[0], quarter.shape[1] // 4
    pieces = [quarter[:, :width]]
    for step in range(1, 4):
        pieces.append(swap_col(quarter[:, step * width : (step + 1) * width], step))
    return place_blocks(pieces, col).reshape(4 * rows, width)


def sum_dp_row(values):
    values = values + swap_dp(values)
    values = values + lax.ppermute(values, "row", CORE_SWAP)
    return values + lax.ppermute(values, "row", CHIP_SWAP)


def seq_attention(query, key_rows, value_rows, seg):
    scores = jnp.einsum("hqd,hkd->hqk", query, key_rows, preferred_element_type=jnp.float32)
    scores = scores * HEAD_DIM ** (-0.5)
    place = jnp.arange(query.shape[1], dtype=jnp.int32)
    allowed = (seg[:, None] == seg[None, :]) & (place[None, :] <= place[:, None])
    scores = jnp.where(allowed[None], scores, masked_score)
    row_max = jnp.max(scores, axis=2, keepdims=True)
    exp_scores = jnp.exp(scores - row_max)
    return exp_scores / jnp.sum(exp_scores, axis=2, keepdims=True)


def body(
    history,
    segment_ids,
    position_ids,
    mix_gain,
    mix_in,
    mix_out,
    mix_bias,
    lane_gain,
    lane_bias,
    qkv_weight,
    qkv_bias,
    proj_weight,
    proj_bias,
    ffn_norm_gain,
    feedforward_norm_bias,
    up_weight,
    up_bias,
    down_weight,
    down_bias,
    cotangent,
):
    f32, bf16 = jnp.float32, jnp.bfloat16
    row, col = lax.axis_index("row"), lax.axis_index("col")
    tok_rows, width = history.shape[1], history.shape[2]
    head_cols = qkv_weight.shape[2]
    heads_local = head_cols // HEAD_DIM
    head_shape = (tok_rows, heads_local, HEAD_DIM)

    qkv_full = [lax.all_gather(qkv_weight[lane], "row", axis=0) for lane in range(3)]
    proj_full = lax.all_gather(proj_weight, "row", axis=0)
    up_full = jnp.concatenate(gather_cols_relative(up_weight), axis=0)
    down_full = jnp.concatenate(gather_cols_relative(down_weight), axis=1)
    qkv_bias_here = pick(lax.all_gather(qkv_bias, "row", axis=0), col).astype(f32)
    ids = lax.all_gather(jnp.concatenate([segment_ids, position_ids], axis=0), "col", axis=0)
    ids = pick(ids, row)
    seg, places = ids[0], ids[1]
    cot_rows = lax.all_gather(split_tokens(cotangent, col), "row", axis=0, tiled=True)

    latest = history[SOURCES - 1].astype(f32)
    gain_mix = mix_gain.astype(f32)
    weight_mix = mix_in.astype(f32)
    mixer_out = mix_out.astype(f32)
    first_stats = jnp.concatenate(
        [
            jnp.dot(latest * gain_mix, weight_mix, precision=highest).T,
            jnp.sum(latest * latest, axis=1)[None, :],
        ],
        axis=0,
    )
    first_stats = small_sum(first_stats, 1)
    mix_scale = lax.rsqrt(first_stats[MIX_HID] / MODEL_WIDTH + mix_eps)
    mix_pre = first_stats[:MIX_HID].T * mix_scale[:, None]
    mix_hidden, mix_gelu_back = jax.vjp(exact_gelu, mix_pre)
    coeffs = (
        jnp.dot(mix_hidden, mixer_out, precision=highest) + mix_bias.astype(f32)
    ).reshape(tok_rows, 4, SOURCES)
    streams = []
    for lane in range(4):
        mixed = coeffs[:, lane, 0:1] * history[0].astype(f32)
        for source in range(1, SOURCES):
            mixed = mixed + coeffs[:, lane, source : source + 1] * history[source].astype(f32)
        streams.append(mixed)
    lane_gains = lane_gain.astype(f32)
    lane_biases = lane_bias.astype(f32)
    norm_stats = small_sum(
        jnp.stack(
            [jnp.sum(streams[lane], axis=1) for lane in range(3)]
            + [jnp.sum(streams[lane] * streams[lane], axis=1) for lane in range(3)],
            axis=0,
        ),
        2,
    )
    units, inv_stds, lane_inputs = [], [], []
    for lane in range(3):
        unit, inv_std = apply_layer_norm(streams[lane], norm_stats[lane], norm_stats[3 + lane])
        units.append(unit)
        inv_stds.append(inv_std)
        lane_inputs.append((unit * lane_gains[lane] + lane_biases[lane]).astype(bf16))

    qkv_pre = []
    for lane in range(3):
        part = jnp.einsum(
            "td,hde->hte", lane_inputs[lane], qkv_full[lane], preferred_element_type=f32
        ).astype(bf16)
        terms = [pick(part, jnp.bitwise_xor(col, step)) for step in range(4)]
        qkv_pre.append(scatter_cols(terms) + qkv_bias_here[lane])
    cosine, sine = rotary_tables(places)
    query = rotate(qkv_pre[0].reshape(head_shape), cosine, sine, 1.0).astype(bf16)
    key_rows = rotate(qkv_pre[1].reshape(head_shape), cosine, sine, 1.0).astype(bf16)
    value_rows = qkv_pre[2].reshape(head_shape).astype(bf16)
    query, key_rows, value_rows = (
        jnp.swapaxes(value, 0, 1) for value in (query, key_rows, value_rows)
    )
    attn_probs = seq_attention(query, key_rows, value_rows, seg)
    probs_low = attn_probs.astype(bf16)
    attended = jnp.einsum("hqk,hkd->qhd", probs_low, value_rows, preferred_element_type=f32)
    attended = attended.astype(bf16).reshape(tok_rows, head_cols)
    attn_full = place_blocks(gather_cols_relative(attended), col)
    attn_proj = jnp.einsum("hte,hed->td", attn_full, proj_full, preferred_element_type=f32)
    resid = streams[3] + attn_proj + proj_bias.astype(f32)

    ffn_gain = ffn_norm_gain.astype(f32)
    ffn_stats = small_sum(
        jnp.stack([jnp.sum(resid, axis=1), jnp.sum(resid * resid, axis=1)], axis=0), 3
    )
    ffn_unit, ffn_inv_std = apply_layer_norm(resid, ffn_stats[0], ffn_stats[1])
    ffn_input = (ffn_unit * ffn_gain + feedforward_norm_bias.astype(f32)).astype(bf16)
    ffn_rows = lax.all_gather(split_tokens(ffn_input, col), "row", axis=0, tiled=True)
    act_grad = jnp.einsum("td,fd->tf", cot_rows, down_full, preferred_element_type=f32)
    up_pre = jnp.dot(ffn_rows, up_full, preferred_element_type=f32) + up_bias.astype(f32)
    up_value, up_gelu_back = jax.vjp(exact_gelu, up_pre)
    up_act = up_value.astype(bf16)
    up_grad = up_gelu_back(act_grad)[0].astype(bf16)
    input_grad = jnp.einsum("tf,df->td", up_grad, up_full, preferred_element_type=f32).astype(bf16)
    input_grad = lax.psum_scatter(input_grad, "row", scatter_dimension=0, tiled=True)
    input_grad = join_tokens(input_grad, col).astype(f32)
    ffn_out = jnp.dot(up_act, down_full, preferred_element_type=f32).astype(bf16)
    ffn_out = lax.psum_scatter(ffn_out, "row", scatter_dimension=0, tiled=True)
    ffn_out = join_tokens(ffn_out, col).astype(f32)
    layer_out = (resid + ffn_out + down_bias.astype(f32)).astype(bf16)

    def over_cols(terms):
        mine = scatter_cols(terms).astype(bf16)
        return low_sum_dp(mine)

    def low_sum_dp(mine):
        return mine.astype(f32) + swap_dp(mine).astype(f32)

    down_terms = jnp.einsum("tf,td->fd", up_act, cot_rows, preferred_element_type=f32).astype(bf16)
    down_weight_grad = over_cols(
        [down_terms[:, step * width : (step + 1) * width] for step in range(4)]
    )
    up_terms = jnp.einsum("td,tf->df", ffn_rows, up_grad, preferred_element_type=f32).astype(bf16)
    up_weight_grad = over_cols(
        [up_terms[step * width : (step + 1) * width] for step in range(4)]
    )
    up_bias_sum = jnp.sum(up_grad, axis=0, dtype=f32).reshape(-1, 512)
    up_bias_sum = up_bias_sum + swap_dp(up_bias_sum)
    up_bias_sum = up_bias_sum + swap_col(up_bias_sum, 1)
    up_bias_grad = (up_bias_sum + swap_col(up_bias_sum, 2)).reshape(-1)

    ffn_scaled = input_grad * ffn_gain
    ffn_back = small_sum(
        jnp.stack([jnp.sum(ffn_scaled, axis=1), jnp.sum(ffn_scaled * ffn_unit, axis=1)], axis=0), 4
    )
    resid_grad = cotangent.astype(f32) + layer_norm_backward(
        input_grad, ffn_unit, ffn_inv_std, ffn_gain, ffn_back[0], ffn_back[1]
    )
    ffn_gain_sum = jnp.sum(input_grad * ffn_unit, axis=0)
    ffn_bias_sum = jnp.sum(input_grad, axis=0)

    proj_grad = resid_grad.astype(bf16)
    attn_part = jnp.einsum("td,hed->hte", proj_grad, proj_full, preferred_element_type=f32)
    attn_part = attn_part.astype(bf16)
    attn_grad = scatter_cols([pick(attn_part, jnp.bitwise_xor(col, step)) for step in range(4)])
    attn_grad = jnp.swapaxes(attn_grad.astype(bf16).reshape(head_shape), 0, 1)
    proj_terms = jnp.einsum("hte,td->hed", attn_full, proj_grad, preferred_element_type=f32)
    proj_weight_grad = low_sum_dp(
        lax.psum_scatter(proj_terms.astype(bf16), "row", scatter_dimension=0, tiled=False)
    )
    probs_grad = jnp.einsum("hqd,hkd->hqk", attn_grad, value_rows, preferred_element_type=f32)
    row_delta = jnp.sum(probs_grad * attn_probs, axis=2, keepdims=True)
    score_grad = (attn_probs * (probs_grad - row_delta)).astype(bf16)
    scale = HEAD_DIM ** (-0.5)
    value_grad = jnp.einsum("hqk,hqd->khd", probs_low, attn_grad, preferred_element_type=f32)
    key_grad = jnp.einsum("hqk,hqd->khd", score_grad, query, preferred_element_type=f32) * scale
    query_grad = jnp.einsum("hqk,hkd->qhd", score_grad, key_rows, preferred_element_type=f32) * scale
    qkv_grad = [
        rotate(query_grad, cosine, sine, -1.0).astype(bf16).reshape(tok_rows, head_cols),
        rotate(key_grad, cosine, sine, -1.0).astype(bf16).reshape(tok_rows, head_cols),
        value_grad.astype(bf16).reshape(tok_rows, head_cols),
    ]
    qkv_grad_full = [None, None, None]
    qkv_terms = [None, None, None]
    for lane in (2, 1, 0):
        qkv_grad_full[lane] = place_blocks(gather_cols_relative(qkv_grad[lane]), col)
        qkv_terms[lane] = lax.psum_scatter(
            jnp.einsum(
                "td,hte->hde", lane_inputs[lane], qkv_grad_full[lane], preferred_element_type=f32
            ).astype(bf16),
            "row",
            scatter_dimension=0,
            tiled=False,
        )
    lane_in_grad = [
        jnp.einsum("hte,hde->td", qkv_grad_full[lane], qkv_full[lane], preferred_element_type=f32)
        for lane in range(3)
    ]
    qkv_weight_grad = jnp.stack([low_sum_dp(qkv_terms[lane]) for lane in range(3)], axis=0)
    qkv_bias_sum = jnp.stack(
        [jnp.sum(qkv_grad_full[lane], axis=1, dtype=f32).reshape(-1) for lane in range(3)], axis=0
    )

    scaled = [lane_in_grad[lane] * lane_gains[lane] for lane in range(3)]
    lane_back = small_sum(
        jnp.stack(
            [jnp.sum(scaled[lane], axis=1) for lane in range(3)]
            + [jnp.sum(scaled[lane] * units[lane], axis=1) for lane in range(3)],
            axis=0,
        ),
        5,
    )
    lane_grads = [
        layer_norm_backward(
            lane_in_grad[lane],
            units[lane],
            inv_stds[lane],
            lane_gains[lane],
            lane_back[lane],
            lane_back[3 + lane],
        )
        for lane in range(3)
    ]
    lane_grads.append(resid_grad)
    lane_gain_sum = [jnp.sum(lane_in_grad[lane] * units[lane], axis=0) for lane in range(3)]
    lane_bias_sum = [jnp.sum(lane_in_grad[lane], axis=0) for lane in range(3)]
    coeff_parts = jnp.stack(
        [
            jnp.sum(lane_grads[lane] * history[source].astype(f32), axis=1)
            for lane in range(4)
            for source in range(SOURCES)
        ],
        axis=0,
    )
    coeff_grad = small_sum(coeff_parts, 6).T
    mix_out_sum = jnp.dot(mix_hidden.T, coeff_grad, precision=highest)
    mix_bias_sum = jnp.sum(coeff_grad, axis=0)
    hidden_grad = jnp.dot(coeff_grad, mixer_out.T, precision=highest)
    pre_grad = mix_gelu_back(hidden_grad)[0]
    normed_mix = latest * mix_scale[:, None] * gain_mix
    mix_in_sum = jnp.dot(normed_mix.T, pre_grad, precision=highest)
    normed_grad = jnp.dot(pre_grad, weight_mix.T, precision=highest)
    mix_gain_sum = jnp.sum(normed_grad * latest * mix_scale[:, None], axis=0)
    weighted = normed_grad * gain_mix
    rms_back = small_sum(jnp.sum(weighted * latest, axis=1)[None, :], 7)
    latest_grad = (
        mix_scale[:, None] * weighted
        - latest
        * (mix_scale * mix_scale * mix_scale)[:, None]
        * (rms_back[0] / MODEL_WIDTH)[:, None]
    )
    source_grads = []
    for source in range(SOURCES):
        summed = coeffs[:, 0, source : source + 1] * lane_grads[0]
        for lane in range(1, 4):
            summed = summed + coeffs[:, lane, source : source + 1] * lane_grads[lane]
        if source == SOURCES - 1:
            summed = summed + latest_grad
        source_grads.append(summed)
    history_grad = jnp.stack(source_grads, axis=0)

    early = jnp.stack(
        [
            ffn_gain_sum,
            ffn_bias_sum,
            jnp.sum(cotangent, axis=0, dtype=f32),
            jnp.sum(proj_grad, axis=0, dtype=f32),
        ],
        axis=0,
    )
    early = sum_dp_row(early)
    middle = jnp.concatenate(
        [qkv_bias_sum.reshape(-1, width), jnp.stack(lane_gain_sum + lane_bias_sum, axis=0)], axis=0
    )
    middle = sum_dp_row(middle)
    bias_blocks = qkv_bias_sum.size // width
    qkv_bias_total = middle[:bias_blocks].reshape(3, -1, head_cols)
    qkv_bias_grad = lax.dynamic_index_in_dim(qkv_bias_total, row, 1, keepdims=False)
    lane_rows = middle[bias_blocks:]
    late = jnp.concatenate(
        [
            mix_in_sum.T,
            mix_gain_sum[None],
            jnp.pad(
                jnp.concatenate([mix_out_sum.reshape(-1), mix_bias_sum]),
                (0, width - MIX_HID * MIX_HID - MIX_HID),
            )[None],
        ],
        axis=0,
    )
    late = sum_dp_row(late)
    return (
        layer_out,
        history_grad,
        late[MIX_HID],
        late[:MIX_HID].T,
        late[MIX_HID + 1, : MIX_HID * MIX_HID].reshape(MIX_HID, MIX_HID),
        late[MIX_HID + 1, MIX_HID * MIX_HID : MIX_HID * MIX_HID + MIX_HID],
        lane_rows[:3],
        lane_rows[3:],
        qkv_weight_grad,
        qkv_bias_grad,
        proj_weight_grad,
        early[3],
        early[0],
        early[1],
        up_weight_grad,
        up_bias_grad,
        down_weight_grad,
        early[2],
    )


def whole_sequence_rows(mesh, args):
    history, segment_ids = args[0], args[1]
    groups = mesh.shape["dp"] * mesh.shape["row"]
    return (
        (mesh.shape["dp"], mesh.shape["row"], mesh.shape["col"]) == (2, 4, 4)
        and history.shape[1] // groups == segment_ids.shape[1]
        and segment_ids.shape[0] == groups
    )


def solution(mesh):
    def program(*args):
        chosen = body if whole_sequence_rows(mesh, args) else general_body
        return sharded(mesh, chosen)(*args)

    return program


def sharded(mesh, chosen):
    return jax.shard_map(
        chosen,
        mesh=mesh,
        in_specs=(
            P(None, ("dp", "row"), "col"),
            P(("dp", "col"), None),
            P(("dp", "col"), None),
            P("col"),
            P("col", None),
            P(),
            P(),
            P(None, "col"),
            P(None, "col"),
            P(None, "col", "row"),
            P(None, "row"),
            P("row", "col"),
            P("col"),
            P("col"),
            P("col"),
            P("col", "row"),
            P("row"),
            P("row", "col"),
            P("col"),
            P(("dp", "row"), "col"),
        ),
        out_specs=(
            P(("dp", "row"), "col"),
            P(None, ("dp", "row"), "col"),
            P("col"),
            P("col", None),
            P(),
            P(),
            P(None, "col"),
            P(None, "col"),
            P(None, "col", "row"),
            P(None, "row"),
            P("row", "col"),
            P("col"),
            P("col"),
            P("col"),
            P("col", "row"),
            P("row"),
            P("row", "col"),
            P("col"),
        ),
        check_vma=False,
    )
```
